16 devices in a mesh: ep: 16 (over z, y, x, core).
Axes of the slice: x: 2, y: 2, z: 2, core: 2. Of those that a mesh axis runs over, the one named last changes fastest.
Arguments:
- tokens: bfloat16 [128, 512, 768], P('ep')
- loss_weight: bfloat16 [128, 512, 768], P('ep')
- w_gate: bfloat16 [768, 64], replicated
- w_in: bfloat16 [64, 768, 3072], P('ep')
- w_out: bfloat16 [64, 3072, 768], P('ep')
- first_expert: int32 [128, 512], P('ep')
- second_expert: int32 [128, 512], P('ep')
- keep_second: int32 [128, 512], P('ep')
Outputs:
- output 1: float32 [], replicated
- output 2: bfloat16 [128, 512, 768], P('ep')
- output 3: bfloat16 [64, 768, 3072], P('ep')
- output 4: bfloat16 [64, 3072, 768], P('ep')
- output 5: float32 [768, 64], replicated
All inputs are finite; a program needn't handle non-finite values.
Results may differ from the reference program's by a relative error of at most 0.00960684.
Values are sent between devices in bfloat16 or wider.
A program may use at most 1 GiB of HBM per device.

```python
import jax
import jax.numpy as jnp
from jax import lax

EXPERTS = 64
HIDDEN = 768
FF_DIM = 3072
SEQ_LEN = 512
GROUPS = 128
CAPACITY = 2 * SEQ_LEN // EXPERTS
TOKENS = GROUPS * SEQ_LEN
NUMEL = TOKENS * HIDDEN
ALPHA = 0.01


def draw_routes(route_key):
    sub_keys = jax.random.split(route_key, 6)
    skew_level = jax.random.randint(sub_keys[0], (GROUPS, 1), 0, 4)
    hot_expert = jax.random.randint(sub_keys[1], (GROUPS, 1), 0, EXPERTS)
    hot_pick = jax.random.randint(sub_keys[2], (GROUPS, SEQ_LEN), 0, 8)
    spread = jax.random.randint(sub_keys[3], (GROUPS, SEQ_LEN), 0, EXPERTS)
    first_expert = jnp.where(hot_pick < skew_level, hot_expert, spread).astype(jnp.int32)
    offset = jax.random.randint(sub_keys[4], (GROUPS, SEQ_LEN), 1, EXPERTS)
    second_expert = ((first_expert + offset) % EXPERTS).astype(jnp.int32)
    keep_second = (jax.random.randint(sub_keys[5], (GROUPS, SEQ_LEN), 0, 3) > 0).astype(jnp.int32)
    return first_expert, second_expert, keep_second


def setup_inputs(seed: int = 0) -> dict:
    sub_keys = jax.random.split(jax.random.key(seed), 6)
    tokens = jax.random.normal(sub_keys[0], (GROUPS, SEQ_LEN, HIDDEN), jnp.float32).astype(jnp.bfloat16)
    loss_weight = jax.random.normal(sub_keys[1], (GROUPS, SEQ_LEN, HIDDEN), jnp.float32).astype(jnp.bfloat16)
    w_gate = (jax.random.normal(sub_keys[2], (HIDDEN, EXPERTS), jnp.float32) * HIDDEN ** -0.5).astype(jnp.bfloat16)
    w_in = (jax.random.normal(sub_keys[3], (EXPERTS, HIDDEN, FF_DIM), jnp.float32) * HIDDEN ** -0.5).astype(jnp.bfloat16)
    w_out = (jax.random.normal(sub_keys[4], (EXPERTS, FF_DIM, HIDDEN), jnp.float32) * FF_DIM ** -0.5).astype(jnp.bfloat16)
    first_expert, second_expert, keep_second = draw_routes(sub_keys[5])
    return {'tokens': tokens, 'loss_weight': loss_weight, 'w_gate': w_gate, 'w_in': w_in, 'w_out': w_out, 'first_expert': first_expert, 'second_expert': second_expert, 'keep_second': keep_second}


def table_for(hot_rows, pos_rows, kept_rows):
    slot_ids = jnp.arange(CAPACITY, dtype=jnp.int32)
    slot_hit = ((pos_rows[:, None, None] == slot_ids) & (kept_rows[:, None, None] > 0)).astype(jnp.float32)
    return hot_rows[:, :, None] * slot_hit


def expert_apply(packed):
    x_slots, w_first, w_second = packed
    pre_act = jnp.einsum('gch,hf->gcf', x_slots.astype(jnp.float32), w_first.astype(jnp.float32))
    act_bf = jax.nn.gelu(pre_act, approximate=True).astype(jnp.bfloat16)
    return jnp.einsum('gcf,fh->gch', act_bf.astype(jnp.float32), w_second.astype(jnp.float32)).astype(jnp.bfloat16)


def reference(tokens, loss_weight, w_gate, w_in, w_out, first_expert, second_expert, keep_second):
    expert_ids = jnp.arange(EXPERTS, dtype=jnp.int32)
    first_int = (first_expert[..., None] == expert_ids).astype(jnp.int32)
    second_int = (second_expert[..., None] == expert_ids).astype(jnp.int32)
    second_keep = second_int * keep_second[..., None]
    first_count = jnp.sum(first_int, axis=1)
    pos_first = jnp.sum((jnp.cumsum(first_int, axis=1) - first_int) * first_int, axis=-1)
    pos_second = jnp.sum((jnp.cumsum(second_keep, axis=1) - second_keep + first_count[:, None, :]) * second_int, axis=-1)
    kept_first = (pos_first < CAPACITY).astype(jnp.int32)
    kept_second = keep_second * (pos_second < CAPACITY).astype(jnp.int32)
    first_hot = first_int.astype(jnp.float32)
    second_hot = second_int.astype(jnp.float32)
    frac_first = jnp.sum(first_hot, axis=(0, 1)) / TOKENS

    def dispatch_group(packed):
        x_group, pos_one, kept_one, hot_one, pos_two, kept_two, hot_two = packed
        table = table_for(hot_one, pos_one, kept_one) + table_for(hot_two, pos_two, kept_two)
        return jnp.einsum('sec,sh->ech', table, x_group).astype(jnp.bfloat16)

    def combine_group(packed):
        y_group, pos_one, kept_one, hot_one, pos_two, kept_two, hot_two, norm_one, norm_two = packed
        combine = (table_for(hot_one, pos_one, kept_one) * norm_one[:, None, None] + table_for(hot_two, pos_two, kept_two) * norm_two[:, None, None]).astype(jnp.bfloat16)
        return jnp.einsum('sec,ech->sh', combine.astype(jnp.float32), y_group.astype(jnp.float32))

    def objective(x_in, gate_w, w_first, w_second):
        x_f32 = x_in.astype(jnp.float32)
        logits = jnp.einsum('gsh,he->gse', x_f32, gate_w)
        router_prob = jax.nn.softmax(logits, axis=-1)
        gate_first = jnp.sum(router_prob * first_hot, axis=-1)
        gate_second = jnp.sum(router_prob * second_hot, axis=-1)
        norm_first = gate_first / (gate_first + gate_second)
        norm_second = gate_second / (gate_first + gate_second)
        slots_in = lax.map(jax.checkpoint(dispatch_group), (x_f32, pos_first, kept_first, first_hot, pos_second, kept_second, second_hot))
        slots_out = lax.map(jax.checkpoint(expert_apply), (jnp.moveaxis(slots_in, 0, 1), w_first, w_second))
        moe_out = lax.map(jax.checkpoint(combine_group), (jnp.moveaxis(slots_out, 0, 1), pos_first, kept_first, first_hot, pos_second, kept_second, second_hot, norm_first, norm_second))
        dot_sum = jnp.sum((x_f32 + moe_out) * loss_weight.astype(jnp.float32))
        mean_prob = jnp.sum(router_prob, axis=(0, 1)) / TOKENS
        loss_value = dot_sum / NUMEL + ALPHA * EXPERTS * jnp.sum(frac_first * mean_prob)
        return loss_value * NUMEL, loss_value

    _, pull_back, loss_value = jax.vjp(objective, tokens, w_gate.astype(jnp.float32), w_in, w_out, has_aux=True)
    grad_x, grad_gate, grad_w_in, grad_w_out = pull_back(jnp.ones((), jnp.float32))
    return loss_value, grad_x, grad_w_in, grad_w_out, grad_gate
```

```python
import functools

import jax
import jax.numpy as jnp
from jax import lax
from jax.experimental import pallas as pl
from jax.experimental.pallas import tpu as pltpu
from jax.sharding import PartitionSpec as P

ALPHA = 0.01
SOURCES = 4
ORDER = (14, 15, 1, 6, 7, 8, 9, 10, 11, 4, 5, 12, 13, 2, 3)
FF_TILE = 768
VMEM_LIMIT = 64 * 1024 * 1024 - 128 * 1024
GELU_K = 0.7978845608028654
GELU_C = 0.044715

BF16 = jnp.bfloat16
F32 = jnp.float32


def dot(a, b, contract=((1,), (0,))):
    return lax.dot_general(a, b, (contract, ((), ())), preferred_element_type=F32)


def route(first_ids, second_ids, keep_ids, experts, cap_rows):
    seq_len = first_ids.shape[1]
    expert_ids = jnp.arange(experts, dtype=jnp.int32)
    first_hot = (first_ids[..., None] == expert_ids).astype(BF16)
    second_hot = (second_ids[..., None] == expert_ids).astype(BF16)
    second_kept = second_hot * keep_ids.astype(BF16)[..., None]
    seq_ids = jnp.arange(seq_len, dtype=jnp.int32)
    earlier = (seq_ids[:, None] > seq_ids[None, :]).astype(BF16)
    before_first = jnp.einsum('st,gte->gse', earlier, first_hot, preferred_element_type=F32)
    before_second = jnp.einsum('st,gte->gse', earlier, second_kept, preferred_element_type=F32)
    first_count = jnp.sum(first_hot, axis=1, dtype=F32)
    pos_first = jnp.sum(before_first * first_hot, axis=-1).astype(jnp.int32)
    pos_second = jnp.sum((before_second + first_count[:, None, :]) * second_hot, axis=-1).astype(jnp.int32)
    slot_first = jnp.where(pos_first < cap_rows, pos_first, -1)
    slot_second = jnp.where((keep_ids == 1) & (pos_second < cap_rows), pos_second, -1)
    return first_hot, second_hot, first_count, slot_first, slot_second


def dispatch_body(l1_ref, l2_ref, x_ref, r_ref, out_ref):
    local, devices, _, _, cap_rows, hidden = out_ref.shape
    slots, seq_len = devices * cap_rows, x_ref.shape[1]
    ids = lax.broadcasted_iota(jnp.int32, (slots, seq_len), 0)
    for j in range(local):
        hit = (l1_ref[0] - j * slots == ids) | (l2_ref[0] - j * slots == ids)
        hot = jnp.where(hit, 1.0, 0.0).astype(BF16)
        for k, ref in enumerate((x_ref, r_ref)):
            out_ref[j, :, k, 0] = dot(hot, ref[0]).astype(BF16).reshape(devices, cap_rows, hidden)


def dispatch(local, devices, cap_rows, l1, l2, x, r):
    groups, seq_len, hidden = x.shape
    slots = local * devices * cap_rows
    id_spec = pl.BlockSpec((1, 1, seq_len), lambda g: (g, 0, 0))
    row_spec = pl.BlockSpec((1, seq_len, hidden), lambda g: (g, 0, 0))
    return pl.pallas_call(
        dispatch_body,
        out_shape=jax.ShapeDtypeStruct((local, devices, 2, groups, cap_rows, hidden), BF16),
        grid=(groups,),
        in_specs=[id_spec, id_spec, row_spec, row_spec],
        out_specs=pl.BlockSpec((local, devices, 2, 1, cap_rows, hidden), lambda g: (0, 0, 0, g, 0, 0)),
        compiler_params=pltpu.CompilerParams(dimension_semantics=('arbitrary',), vmem_limit_bytes=VMEM_LIMIT),
        cost_estimate=pl.CostEstimate(flops=4 * groups * slots * seq_len * hidden, bytes_accessed=4 * x.size + 4 * groups * slots * hidden, transcendentals=0),
        name='dispatch',
    )(l1[:, None, :], l2[:, None, :], x, r)


def moe_body(ff_tile, send_ref, nstat_ref, w1_ref, w2_ref, recv_ref, dxs_ref, back_ref, dw1_ref, dw2_ref, dsend_ref, dback_ref, stat_ref,
             w1_buf, w2_buf, acc1, acc2, tile, dx_tile, nrecv, dwin,
             in_send, in_recv, out_send, out_recv, n_send, n_recv, d_send, d_recv, w_sem, x_sem, dx_sem, dw_sem, own_sem):
    local, devices, both, hidden = send_ref.shape
    window = both // 2
    ff = w1_ref.shape[2]
    rows = SOURCES * window
    tiles = devices // SOURCES
    me = lax.axis_index('ep')

    core, chip = lax.rem(me, 2), me // 2
    bits = [lax.rem(chip // b, 2) for b in (1, 2, 4)]

    def peer_of(k):
        out = me + (1 - 2 * core) * (k % 2)
        for n, bit in enumerate(bits):
            out = out + 2 ** (n + 1) * (1 - 2 * bit) * (k // 2 ** (n + 1) % 2)
        return out

    def remote(src, dst, s, r, peer):
        return pltpu.make_async_remote_copy(src_ref=src, dst_ref=dst, send_sem=s, recv_sem=r, device_id=(peer,), device_id_type=pl.DeviceIdType.MESH)

    def in_copy(j, k, peer):
        return remote(send_ref.at[j, peer], recv_ref.at[j, me], in_send.at[j, k], in_recv.at[j, k], peer)

    def in_landing(j, k, peer):
        return remote(send_ref.at[j, peer], recv_ref.at[j, peer], in_send.at[j, k], in_recv.at[j, k], peer)

    def out_copy(j, k, peer):
        return remote(dxs_ref.at[j, peer], back_ref.at[j, me], out_send.at[j, k], out_recv.at[j, k], peer)

    def out_landing(j, k, peer):
        return remote(dxs_ref.at[j, peer], back_ref.at[j, peer], out_send.at[j, k], out_recv.at[j, k], peer)

    def n_copy(k, peer):
        return remote(nstat_ref.at[peer], nrecv.at[me], n_send.at[k], n_recv.at[k], peer)

    def n_landing(k, peer):
        return remote(nstat_ref.at[peer], nrecv.at[peer], n_send.at[k], n_recv.at[k], peer)

    def d_copy(k, peer):
        return remote(dsend_ref.at[peer], dback_ref.at[me], d_send.at[k], d_recv.at[k], peer)

    def d_landing(k, peer):
        return remote(dsend_ref.at[peer], dback_ref.at[peer], d_send.at[k], d_recv.at[k], peer)

    def each_peer(fn):
        for k in ORDER:
            fn(k, peer_of(k))

    def start_in(j):
        each_peer(lambda k, peer: in_copy(j, k, peer).start())

    def members(t):
        on = [jnp.where(t == 3 - n, 1, 0) for n in range(3)]
        near = chip + sum(2 ** n * (1 - 2 * bits[n]) * on[n] for n in range(3))
        key = sum(2 ** n * on[n] for n in range(3))
        out = []
        for c, q in ((7 - near, 7 - key), (near, key)):
            out += [(2 * q, 2 * c + core), (2 * q + 1, 2 * c + 1 - core)]
        return out

    def weight_copies(j, slot):
        return (pltpu.make_async_copy(w1_ref.at[j], w1_buf.at[slot], w_sem.at[slot, 0]),
                pltpu.make_async_copy(w2_ref.at[j], w2_buf.at[slot], w_sem.at[slot, 1]))

    def tile_copy(j, s, p, ref):
        return pltpu.make_async_copy(ref.at[j, s], tile.at[p], x_sem.at[p])

    def grad_copies(j, slot):
        return (pltpu.make_async_copy(w1_buf.at[slot], dw1_ref.at[j], dw_sem.at[slot, 0]),
                pltpu.make_async_copy(w2_buf.at[slot], dw2_ref.at[j], dw_sem.at[slot, 1]))

    each_peer(lambda k, peer: n_copy(k, peer).start())
    own = pltpu.make_async_copy(nstat_ref.at[me], nrecv.at[me], own_sem)
    own.start()
    for j in range(local):
        start_in(j)
    for copy in weight_copies(0, 0):
        copy.start()
    own.wait()
    each_peer(lambda k, peer: n_landing(k, peer).wait())
    stat_ref[...] = jnp.sum(nrecv[...], axis=0)
    diag = lax.broadcasted_iota(jnp.int32, (window, window), 0) == lax.broadcasted_iota(jnp.int32, (window, window), 1)

    @pl.loop(0, local * tiles)
    def _(i):
        j = i // tiles
        t = lax.rem(i, tiles)
        wslot = lax.rem(j, 2)
        slot = lax.rem(i, 2)
        sources = members(t)

        @pl.when(t == 0)
        def _():
            for copy in weight_copies(j, wslot):
                copy.wait()
            acc1[...] = jnp.zeros_like(acc1)
            acc2[...] = jnp.zeros_like(acc2)

        @pl.when((t == 1) & (j > 0))
        def _():
            for copy in grad_copies(j - 1, 1 - wslot):
                copy.wait()

        @pl.when((t == 1) & (j + 1 < local))
        def _():
            for copy in weight_copies(j + 1, 1 - wslot):
                copy.start()

        for p, (k, s) in enumerate(sources):
            if p == 2:
                @pl.when(t == 0)
                def _():
                    tile_copy(j, s, p, send_ref).start()

                @pl.when(t > 0)
                def _():
                    in_landing(j, k, s).wait_recv()
                    tile_copy(j, s, p, recv_ref).start()
            else:
                in_landing(j, k, s).wait_recv()
                tile_copy(j, s, p, recv_ref).start()
        for p, (k, s) in enumerate(sources):
            tile_copy(j, s, p, recv_ref).wait()

        x = tile[:, :window].reshape(rows, hidden)
        r = tile[:, window:].reshape(rows, hidden).astype(F32)
        weights = [jnp.sum(jnp.where(diag, nrecv[s, pl.ds(j, 1), :], 0.0), axis=1, keepdims=True) for _, s in sources]
        g = (r * jnp.concatenate(weights, axis=0)).astype(BF16)
        h = None
        dx = None
        for f0 in range(0, ff, ff_tile):
            w1 = w1_buf[wslot, :, f0:f0 + ff_tile]
            w2 = w2_buf[wslot, f0:f0 + ff_tile, :]
            pre = dot(x, w1)
            sq = pre * pre
            th = jnp.tanh(pre * (GELU_K + (GELU_K * GELU_C) * sq))
            half = 0.5 + 0.5 * th
            act = (pre * half).astype(BF16)
            slope = half + (0.5 * pre) * (1.0 - th * th) * (GELU_K + (3.0 * GELU_K * GELU_C) * sq)
            ga = dot(g, w2, ((1,), (1,))).astype(BF16).astype(F32)
            gp = (ga * slope).astype(BF16)
            hp = dot(act, w2)
            h = hp if h is None else h + hp
            dp = dot(gp, w1, ((1,), (1,)))
            dx = dp if dx is None else dx + dp
            acc1[:, f0:f0 + ff_tile] += dot(x, gp, ((0,), (0,)))
            acc2[f0:f0 + ff_tile, :] += dot(act, g, ((0,), (0,)))
        dx_tile[slot] = dx.astype(BF16).reshape(SOURCES, window, hidden)
        stores = [pltpu.make_async_copy(dx_tile.at[slot, p], dxs_ref.at[j, s], dx_sem.at[p]) for p, (_, s) in enumerate(sources)]
        for p, copy in enumerate(stores):
            if p != 2:
                copy.start()

        @pl.when(t > 0)
        def _():
            stores[2].start()

        @pl.when(t == 0)
        def _():
            kept = pltpu.make_async_copy(dx_tile.at[slot, 2], back_ref.at[j, me], dx_sem.at[2])
            kept.start()

        d = jnp.sum(r * h.astype(BF16).astype(F32), axis=1, keepdims=True)
        for p, (_, s) in enumerate(sources):
            dwin[s, pl.ds(j, 1), :] = jnp.sum(jnp.where(diag, d[p * window:(p + 1) * window], 0.0), axis=0, keepdims=True)
        for p, (k, s) in enumerate(sources):
            stores[p].wait()
            if p == 2:
                @pl.when(t > 0)
                def _():
                    out_copy(j, k, s).start()
            else:
                out_copy(j, k, s).start()

        @pl.when(t == tiles - 1)
        def _():
            w1_buf[wslot] = acc1[...].astype(BF16)
            w2_buf[wslot] = acc2[...].astype(BF16)
            for copy in grad_copies(j, wslot):
                copy.start()

    saved = pltpu.make_async_copy(dwin, dsend_ref, own_sem)
    saved.start()
    saved.wait()
    each_peer(lambda k, peer: d_copy(k, peer).start())
    own = pltpu.make_async_copy(dwin.at[me], dback_ref.at[me], own_sem)
    own.start()
    own.wait()
    for copy in grad_copies(local - 1, (local - 1) % 2):
        copy.wait()
    each_peer(lambda k, peer: d_landing(k, peer).wait())

    @pl.loop(0, local)
    def _(j):
        each_peer(lambda k, peer: in_copy(j, k, peer).wait_send())
        each_peer(lambda k, peer: out_landing(j, k, peer).wait())


def moe(send, nstat, w_in, w_out):
    local, devices, both, hidden = send.shape
    window = both // 2
    ff = w_in.shape[2]
    anywhere = pl.BlockSpec(memory_space=pl.ANY)
    slots = jax.ShapeDtypeStruct((local, devices, window, hidden), BF16)
    small = jax.ShapeDtypeStruct(nstat.shape, F32)
    dma = pltpu.SemaphoreType.DMA
    return pl.pallas_call(
        functools.partial(moe_body, FF_TILE),
        out_shape=(
            jax.ShapeDtypeStruct(send.shape, BF16), slots, slots,
            jax.ShapeDtypeStruct(w_in.shape, BF16), jax.ShapeDtypeStruct(w_out.shape, BF16),
            small, small, jax.ShapeDtypeStruct(nstat.shape[1:], F32),
        ),
        in_specs=[anywhere] * 4,
        out_specs=(anywhere,) * 7 + (pl.BlockSpec(memory_space=pltpu.VMEM),),
        scratch_shapes=[
            pltpu.VMEM((2, hidden, ff), BF16), pltpu.VMEM((2, ff, hidden), BF16),
            pltpu.VMEM((hidden, ff), F32), pltpu.VMEM((ff, hidden), F32),
            pltpu.VMEM((SOURCES, both, hidden), BF16), pltpu.VMEM((2, SOURCES, window, hidden), BF16),
            pltpu.VMEM(nstat.shape, F32), pltpu.VMEM(nstat.shape, F32),
            dma((local, devices)), dma((local, devices)), dma((local, devices)), dma((local, devices)),
            dma((devices,)), dma((devices,)), dma((devices,)), dma((devices,)),
            dma((2, 2)), dma((SOURCES,)), dma((SOURCES,)), dma((2, 2)), dma,
        ],
        compiler_params=pltpu.CompilerParams(has_side_effects=True, vmem_limit_bytes=VMEM_LIMIT),
        cost_estimate=pl.CostEstimate(flops=12 * local * devices * window * hidden * ff, bytes_accessed=8 * local * hidden * ff, transcendentals=local * devices * window * ff),
        name='moe',
    )(send, nstat, w_in, w_out)


def combine_body(l1_ref, l2_ref, back_ref, res_ref, gl_ref, wg_ref, out_ref):
    local, devices, _, cap_rows, hidden = back_ref.shape
    seq_len = l1_ref.shape[2]
    slots = local * devices * cap_rows
    ids = lax.broadcasted_iota(jnp.int32, (slots, seq_len), 0)
    hit = (l1_ref[0] == ids) | (l2_ref[0] == ids)
    hot = jnp.where(hit, 1.0, 0.0).astype(BF16)
    total = dot(hot, back_ref[...].reshape(slots, hidden), ((0,), (0,)))
    total += res_ref[0].astype(F32)
    total += dot(gl_ref[0], wg_ref[...], ((1,), (1,)))
    out_ref[0] = total.astype(out_ref.dtype)


def combine(l1, l2, back, res, grad_logits, w_gate):
    groups, seq_len, hidden = res.shape
    local, devices, _, cap_rows, _ = back.shape
    slots = local * devices * cap_rows
    experts = w_gate.shape[1]
    id_spec = pl.BlockSpec((1, 1, seq_len), lambda g: (g, 0, 0))
    row_spec = pl.BlockSpec((1, seq_len, hidden), lambda g: (g, 0, 0))
    return pl.pallas_call(
        combine_body,
        out_shape=jax.ShapeDtypeStruct(res.shape, BF16),
        grid=(groups,),
        in_specs=[
            id_spec, id_spec, pl.BlockSpec((local, devices, 1, cap_rows, hidden), lambda g: (0, 0, g, 0, 0)), row_spec,
            pl.BlockSpec((1, seq_len, experts), lambda g: (g, 0, 0)), pl.BlockSpec((hidden, experts), lambda g: (0, 0)),
        ],
        out_specs=row_spec,
        compiler_params=pltpu.CompilerParams(dimension_semantics=('arbitrary',), vmem_limit_bytes=VMEM_LIMIT),
        cost_estimate=pl.CostEstimate(flops=2 * groups * slots * seq_len * hidden, bytes_accessed=2 * groups * slots * hidden + 6 * res.size, transcendentals=0),
        name='combine',
    )(l1[:, None, :], l2[:, None, :], back, res, grad_logits, w_gate)


def solution(mesh):
    ep_size = mesh.shape['ep']

    def layer_body(x_loc, r_loc, w_gate, w_in_loc, w_out_loc, first_ids, second_ids, keep_ids):
        local_groups, seq_len, hidden = x_loc.shape
        experts = w_gate.shape[1]
        local = experts // ep_size
        cap_rows = 2 * seq_len // experts
        region = local_groups * cap_rows
        tokens_all = local_groups * ep_size * seq_len
        numel = tokens_all * hidden

        first_hot, second_hot, first_count, slot_first, slot_second = route(first_ids, second_ids, keep_ids, experts, cap_rows)

        def slot_of(slot, expert_of):
            return jnp.where(slot >= 0, ((expert_of % local) * ep_size + expert_of // local) * cap_rows + slot, -1)

        l1, l2 = slot_of(slot_first, first_ids), slot_of(slot_second, second_ids)
        send = dispatch(local, ep_size, cap_rows, l1, l2, x_loc, r_loc).reshape(local, ep_size, 2 * region, hidden)

        logits = jnp.einsum('gsh,he->gse', x_loc, w_gate, preferred_element_type=F32)
        router_prob = jax.nn.softmax(logits, axis=-1)
        gate_first = jnp.sum(router_prob * first_hot, axis=-1)
        gate_second = jnp.sum(router_prob * second_hot, axis=-1)
        gate_sum = gate_first + gate_second
        norm_first = (gate_first / gate_sum).astype(BF16)
        norm_second = (gate_second / gate_sum).astype(BF16)
        slot_ids = jnp.arange(cap_rows, dtype=jnp.int32)
        slot_hot_first = (slot_first[..., None] == slot_ids).astype(BF16)
        slot_hot_second = (slot_second[..., None] == slot_ids).astype(BF16)
        nwin = (jnp.einsum('gse,gsc->egc', first_hot, slot_hot_first * norm_first[..., None], preferred_element_type=F32)
                + jnp.einsum('gse,gsc->egc', second_hot, slot_hot_second * norm_second[..., None], preferred_element_type=F32))
        stats = jnp.concatenate([jnp.sum(first_count, axis=0), jnp.sum(router_prob, axis=(0, 1))])
        nwin_rows = nwin.reshape(ep_size, local, region)
        stat_rows = jnp.broadcast_to(jnp.pad(stats, (0, region - 2 * experts)), (ep_size, 1, region))
        nstat = jnp.concatenate([nwin_rows, stat_rows, jnp.zeros((ep_size, 7 - local, region), F32)], axis=1)
        _, _, back, dw1, dw2, _, dback, stats = moe(send, nstat, w_in_loc, w_out_loc)
        frac_first = stats[local, :experts] / tokens_all
        mean_prob = stats[local, experts:2 * experts] / tokens_all
        dwin = dback[:, :local].reshape(experts, local_groups, cap_rows)
        dot_sum = jnp.einsum('gsh,gsh->', x_loc, r_loc, preferred_element_type=F32) + jnp.sum(nwin * dwin)
        dwin_bf = dwin.astype(BF16)
        d_first = jnp.einsum('gse,egc->gsc', first_hot, dwin_bf, preferred_element_type=F32)
        d_second = jnp.einsum('gse,egc->gsc', second_hot, dwin_bf, preferred_element_type=F32)
        grad_norm_first = jnp.sum(d_first * slot_hot_first, axis=-1)
        grad_norm_second = jnp.sum(d_second * slot_hot_second, axis=-1)
        gate_sq = gate_sum * gate_sum
        grad_gate_first = (grad_norm_first - grad_norm_second) * gate_second / gate_sq
        grad_gate_second = (grad_norm_second - grad_norm_first) * gate_first / gate_sq
        grad_prob = grad_gate_first[..., None] * first_hot + grad_gate_second[..., None] * second_hot + (ALPHA * hidden * experts) * frac_first
        grad_logits = router_prob * (grad_prob - jnp.sum(router_prob * grad_prob, axis=-1, keepdims=True))
        grad_logits_bf = grad_logits.astype(BF16)
        grad_gate_local = jnp.einsum('gsh,gse->he', x_loc, grad_logits_bf, preferred_element_type=F32)
        grad_gate_w, dot_all = lax.psum((grad_gate_local, dot_sum[None]), 'ep')
        loss_value = dot_all[0] / numel + ALPHA * experts * jnp.sum(frac_first * mean_prob)

        grad_x = combine(l1, l2, back.reshape(local, ep_size, local_groups, cap_rows, hidden), r_loc, grad_logits_bf, w_gate)
        return loss_value, grad_x, dw1, dw2, grad_gate_w

    row_spec = P('ep', None, None)
    id_spec = P('ep', None)
    return jax.shard_map(layer_body, mesh=mesh, in_specs=(row_spec, row_spec, P(None, None), row_spec, row_spec, id_spec, id_spec, id_spec), out_specs=(P(), row_spec, row_spec, row_spec, P(None, None)), check_vma=False)
```

```python
import functools

import jax
import jax.numpy as jnp
from jax import lax
from jax.experimental import pallas as pl
from jax.experimental.pallas import tpu as pltpu
from jax.sharding import PartitionSpec as P

ALPHA = 0.01
SOURCES = 4
LATE = 2
ORDER = (14, 15, 1, 6, 7, 8, 9, 10, 11, 4, 5, 12, 13, 2, 3)
FF_TILE = 768
VMEM_LIMIT = 64 * 1024 * 1024 - 128 * 1024
GELU_K = 0.7978845608028654
GELU_C = 0.044715

BF16 = jnp.bfloat16
F32 = jnp.float32


def dot(a, b, contract=((1,), (0,))):
    return lax.dot_general(a, b, (contract, ((), ())), preferred_element_type=F32)


def route(first_ids, second_ids, keep_ids, experts, cap_rows):
    seq_len = first_ids.shape[1]
    expert_ids = jnp.arange(experts, dtype=jnp.int32)
    first_hot = (first_ids[..., None] == expert_ids).astype(BF16)
    second_hot = (second_ids[..., None] == expert_ids).astype(BF16)
    second_kept = second_hot * keep_ids.astype(BF16)[..., None]
    seq_ids = jnp.arange(seq_len, dtype=jnp.int32)
    earlier = (seq_ids[:, None] > seq_ids[None, :]).astype(BF16)
    before_first = jnp.einsum('st,gte->gse', earlier, first_hot, preferred_element_type=F32)
    before_second = jnp.einsum('st,gte->gse', earlier, second_kept, preferred_element_type=F32)
    first_count = jnp.sum(first_hot, axis=1, dtype=F32)
    pos_first = jnp.sum(before_first * first_hot, axis=-1).astype(jnp.int32)
    pos_second = jnp.sum((before_second + first_count[:, None, :]) * second_hot, axis=-1).astype(jnp.int32)
    slot_first = jnp.where(pos_first < cap_rows, pos_first, -1)
    slot_second = jnp.where((keep_ids == 1) & (pos_second < cap_rows), pos_second, -1)
    return first_hot, second_hot, first_count, slot_first, slot_second


def moe_body(ff_tile, l1_ref, l2_ref, xg_ref, rg_ref, nstat_ref, w1_ref, w2_ref, send_ref, recv_ref, dxs_ref, late_ref, back_ref, dw1_ref, dw2_ref, dsend_ref, dback_ref, stat_ref,
             w1_buf, w2_buf, acc1, acc2, tile, dx_tile, nrecv, dwin,
             in_send, in_recv, out_send, out_recv, n_send, n_recv, d_send, d_recv, w_sem, x_sem, dx_sem, dw_sem, own_sem, load_sem):
    local, devices, _, groups, cap_rows, hidden = send_ref.shape
    window = groups * cap_rows
    seq_len = xg_ref.shape[1]
    ff = w1_ref.shape[2]
    early = dxs_ref.shape[0]
    rows = SOURCES * window
    tiles = devices // SOURCES
    me = lax.axis_index('ep')

    core, chip = lax.rem(me, 2), me // 2
    bits = [lax.rem(chip // b, 2) for b in (1, 2, 4)]

    def peer_of(k):
        out = me + (1 - 2 * core) * (k % 2)
        for n, bit in enumerate(bits):
            out = out + 2 ** (n + 1) * (1 - 2 * bit) * (k // 2 ** (n + 1) % 2)
        return out

    def remote(src, dst, s, r, peer):
        return pltpu.make_async_remote_copy(src_ref=src, dst_ref=dst, send_sem=s, recv_sem=r, device_id=(peer,), device_id_type=pl.DeviceIdType.MESH)

    def in_copy(j, k, peer):
        return remote(send_ref.at[j, peer], recv_ref.at[j, me], in_send.at[j, k], in_recv.at[j, k], peer)

    def in_landing(j, k, peer):
        return remote(send_ref.at[j, peer], recv_ref.at[j, peer], in_send.at[j, k], in_recv.at[j, k], peer)

    def out_copy(j, k, peer):
        return remote(dxs_ref.at[j, peer], back_ref.at[j, me], out_send.at[j, k], out_recv.at[j, k], peer)

    def out_landing(j, k, peer):
        return remote(dxs_ref.at[j, peer], back_ref.at[j, peer], out_send.at[j, k], out_recv.at[j, k], peer)

    def n_copy(k, peer):
        return remote(nstat_ref.at[peer], nrecv.at[me], n_send.at[k], n_recv.at[k], peer)

    def n_landing(k, peer):
        return remote(nstat_ref.at[peer], nrecv.at[peer], n_send.at[k], n_recv.at[k], peer)

    def d_copy(k, peer):
        return remote(dsend_ref.at[peer], dback_ref.at[me], d_send.at[k], d_recv.at[k], peer)

    def d_landing(k, peer):
        return remote(dsend_ref.at[peer], dback_ref.at[peer], d_send.at[k], d_recv.at[k], peer)

    def each_peer(fn):
        for k in ORDER:
            fn(k, peer_of(k))

    def start_in(j):
        each_peer(lambda k, peer: in_copy(j, k, peer).start())

    def members(t):
        on = [jnp.where(t == 3 - n, 1, 0) for n in range(3)]
        near = chip + sum(2 ** n * (1 - 2 * bits[n]) * on[n] for n in range(3))
        key = sum(2 ** n * on[n] for n in range(3))
        out = []
        for c, q in ((7 - near, 7 - key), (near, key)):
            out += [(2 * q, 2 * c + core), (2 * q + 1, 2 * c + 1 - core)]
        return out

    def weight_copies(j, slot):
        return (pltpu.make_async_copy(w1_ref.at[j], w1_buf.at[slot], w_sem.at[slot, 0]),
                pltpu.make_async_copy(w2_ref.at[j], w2_buf.at[slot], w_sem.at[slot, 1]))

    def tile_copy(j, s, p, ref):
        return pltpu.make_async_copy(ref.at[j, s], tile.at[p], x_sem.at[p])

    def grad_copies(j, slot):
        return (pltpu.make_async_copy(w1_buf.at[slot], dw1_ref.at[j], dw_sem.at[slot, 0]),
                pltpu.make_async_copy(w2_buf.at[slot], dw2_ref.at[j], dw_sem.at[slot, 1]))

    each_peer(lambda k, peer: n_copy(k, peer).start())
    own = pltpu.make_async_copy(nstat_ref.at[me], nrecv.at[me], own_sem)
    own.start()

    held = w2_buf.shape[1] // seq_len
    x_at = [w2_buf.at[g // held, pl.ds(g % held * seq_len, seq_len)] for g in range(groups)]
    wide = ff // hidden
    r_at = [w1_buf.at[g // wide, pl.ds(0, seq_len), pl.ds(g % wide * hidden, hidden)] for g in range(groups)]
    loads = [(pltpu.make_async_copy(xg_ref.at[g], x_at[g], load_sem.at[g, 0]), pltpu.make_async_copy(rg_ref.at[g], r_at[g], load_sem.at[g, 1])) for g in range(groups)]
    for pair in loads:
        for copy in pair:
            copy.start()
    slots = devices * cap_rows
    ids = lax.broadcasted_iota(jnp.int32, (slots, seq_len), 0)

    @pl.loop(0, local)
    def _(j):
        def placed(g, k):
            return pltpu.make_async_copy(dx_tile.at[g % 2, k], send_ref.at[j, :, k, g], dx_sem.at[g % 2 * 2 + k])

        for g in range(groups):
            @pl.when(j == 0)
            def _():
                for copy in loads[g]:
                    copy.wait()

            hit = (l1_ref[g] - j * slots == ids) | (l2_ref[g] - j * slots == ids)
            hot = jnp.where(hit, 1.0, 0.0).astype(BF16)
            for k, src in enumerate((x_at[g], r_at[g])):
                value = dot(hot, src[...]).astype(BF16).reshape(devices, cap_rows, hidden)
                if g >= 2:
                    placed(g - 2, k).wait()
                dx_tile[g % 2, k] = value
                placed(g, k).start()
        for g in (groups - 2, groups - 1):
            for k in range(2):
                placed(g, k).wait()
        start_in(j)

    for copy in weight_copies(0, 0):
        copy.start()
    own.wait()
    each_peer(lambda k, peer: n_landing(k, peer).wait())
    stat_ref[...] = jnp.sum(nrecv[...], axis=0)
    diag = lax.broadcasted_iota(jnp.int32, (window, window), 0) == lax.broadcasted_iota(jnp.int32, (window, window), 1)

    @pl.loop(0, local * tiles)
    def _(i):
        j = i // tiles
        t = lax.rem(i, tiles)
        wslot = lax.rem(j, 2)
        slot = lax.rem(i, 2)
        sources = members(t)

        @pl.when(t == 0)
        def _():
            for copy in weight_copies(j, wslot):
                copy.wait()
            acc1[...] = jnp.zeros_like(acc1)
            acc2[...] = jnp.zeros_like(acc2)

        @pl.when((t == 1) & (j > 0))
        def _():
            for copy in grad_copies(j - 1, 1 - wslot):
                copy.wait()

        @pl.when((t == 1) & (j + 1 < local))
        def _():
            for copy in weight_copies(j + 1, 1 - wslot):
                copy.start()

        for p, (k, s) in enumerate(sources):
            if p == 2:
                @pl.when(t == 0)
                def _():
                    tile_copy(j, s, p, send_ref).start()

                @pl.when(t > 0)
                def _():
                    in_landing(j, k, s).wait_recv()
                    tile_copy(j, s, p, recv_ref).start()
            else:
                in_landing(j, k, s).wait_recv()
                tile_copy(j, s, p, recv_ref).start()
        for p, (k, s) in enumerate(sources):
            tile_copy(j, s, p, recv_ref).wait()

        x = tile[:, 0].reshape(rows, hidden)
        r = tile[:, 1].reshape(rows, hidden).astype(F32)
        weights = [jnp.sum(jnp.where(diag, nrecv[s, pl.ds(j, 1), :], 0.0), axis=1, keepdims=True) for _, s in sources]
        g = (r * jnp.concatenate(weights, axis=0)).astype(BF16)
        h = None
        dx = None
        for f0 in range(0, ff, ff_tile):
            w1 = w1_buf[wslot, :, f0:f0 + ff_tile]
            w2 = w2_buf[wslot, f0:f0 + ff_tile, :]
            pre = dot(x, w1)
            sq = pre * pre
            th = jnp.tanh(pre * (GELU_K + (GELU_K * GELU_C) * sq))
            half = 0.5 + 0.5 * th
            act = (pre * half).astype(BF16)
            slope = half + (0.5 * pre) * (1.0 - th * th) * (GELU_K + (3.0 * GELU_K * GELU_C) * sq)
            ga = dot(g, w2, ((1,), (1,))).astype(BF16).astype(F32)
            gp = (ga * slope).astype(BF16)
            hp = dot(act, w2)
            h = hp if h is None else h + hp
            dp = dot(gp, w1, ((1,), (1,)))
            dx = dp if dx is None else dx + dp
            acc1[:, f0:f0 + ff_tile] += dot(x, gp, ((0,), (0,)))
            acc2[f0:f0 + ff_tile, :] += dot(act, g, ((0,), (0,)))
        dx_tile[slot] = dx.astype(BF16).reshape(dx_tile.shape[1:])
        def store(p, dst):
            return pltpu.make_async_copy(dx_tile.at[slot, p // 2, pl.ds(p % 2 * groups, groups)], dst, dx_sem.at[p])

        @pl.when(j < early)
        def _():
            for p, (_, s) in enumerate(sources):
                if p == 2:
                    @pl.when(t == 0)
                    def _():
                        store(p, back_ref.at[j, me]).start()

                    @pl.when(t > 0)
                    def _():
                        store(p, dxs_ref.at[j, s]).start()
                else:
                    store(p, dxs_ref.at[j, s]).start()

        @pl.when(j >= early)
        def _():
            for p, (_, s) in enumerate(sources):
                store(p, late_ref.at[s, j - early]).start()

        d = jnp.sum(r * h.astype(BF16).astype(F32), axis=1, keepdims=True)
        for p, (_, s) in enumerate(sources):
            dwin[s, pl.ds(j, 1), :] = jnp.sum(jnp.where(diag, d[p * window:(p + 1) * window], 0.0), axis=0, keepdims=True)
        for p, (k, s) in enumerate(sources):
            store(p, late_ref.at[s, 0]).wait()
            if p == 2:
                @pl.when((j < early) & (t > 0))
                def _():
                    out_copy(j, k, s).start()
            else:
                @pl.when(j < early)
                def _():
                    out_copy(j, k, s).start()

        @pl.when(t == tiles - 1)
        def _():
            w1_buf[wslot] = acc1[...].astype(BF16)
            w2_buf[wslot] = acc2[...].astype(BF16)
            for copy in grad_copies(j, wslot):
                copy.start()

    saved = pltpu.make_async_copy(dwin, dsend_ref, own_sem)
    saved.start()
    saved.wait()
    each_peer(lambda k, peer: d_copy(k, peer).start())
    own = pltpu.make_async_copy(dwin.at[me], dback_ref.at[me], own_sem)
    own.start()
    own.wait()
    for copy in grad_copies(local - 1, (local - 1) % 2):
        copy.wait()
    each_peer(lambda k, peer: d_landing(k, peer).wait())

    @pl.loop(0, local)
    def _(j):
        each_peer(lambda k, peer: in_copy(j, k, peer).wait_send())

        @pl.when(j < early)
        def _():
            each_peer(lambda k, peer: out_landing(j, k, peer).wait())


def moe(l1, l2, x, r, nstat, w_in, w_out, cap_rows):
    local, hidden, ff = w_in.shape
    devices = nstat.shape[0]
    groups = x.shape[0]
    early = local - LATE
    anywhere = pl.BlockSpec(memory_space=pl.ANY)
    vmem = pl.BlockSpec(memory_space=pltpu.VMEM)
    region = (groups, cap_rows, hidden)
    send = jax.ShapeDtypeStruct((local, devices, 2) + region, BF16)
    slots = jax.ShapeDtypeStruct((early, devices) + region, BF16)
    late = jax.ShapeDtypeStruct((devices, LATE) + region, BF16)
    small = jax.ShapeDtypeStruct(nstat.shape, F32)
    dma = pltpu.SemaphoreType.DMA
    rows = devices * groups * cap_rows
    return pl.pallas_call(
        functools.partial(moe_body, FF_TILE),
        out_shape=(
            send, send, slots, late, slots,
            jax.ShapeDtypeStruct(w_in.shape, BF16), jax.ShapeDtypeStruct(w_out.shape, BF16),
            small, small, jax.ShapeDtypeStruct(nstat.shape[1:], F32),
        ),
        in_specs=[vmem] * 2 + [anywhere] * 5,
        out_specs=(anywhere,) * 9 + (vmem,),
        scratch_shapes=[
            pltpu.VMEM((2, hidden, ff), BF16), pltpu.VMEM((2, ff, hidden), BF16),
            pltpu.VMEM((hidden, ff), F32), pltpu.VMEM((ff, hidden), F32),
            pltpu.VMEM((SOURCES, 2) + region, BF16), pltpu.VMEM((2, 2, devices, cap_rows, hidden), BF16),
            pltpu.VMEM(nstat.shape, F32), pltpu.VMEM(nstat.shape, F32),
            dma((local, devices)), dma((local, devices)), dma((early, devices)), dma((early, devices)),
            dma((devices,)), dma((devices,)), dma((devices,)), dma((devices,)),
            dma((2, 2)), dma((SOURCES,)), dma((SOURCES,)), dma((2, 2)), dma, dma((groups, 2)),
        ],
        compiler_params=pltpu.CompilerParams(has_side_effects=True, vmem_limit_bytes=VMEM_LIMIT),
        cost_estimate=pl.CostEstimate(flops=12 * local * rows * hidden * ff, bytes_accessed=8 * local * hidden * ff, transcendentals=local * rows * ff),
        name='moe',
    )(l1[:, None, :], l2[:, None, :], x, r, nstat, w_in, w_out)


def combine_body(l1_ref, l2_ref, early_ref, late_ref, res_ref, gl_ref, wg_ref, out_ref):
    early, devices, _, cap_rows, hidden = early_ref.shape
    seq_len = l1_ref.shape[2]
    slots = devices * cap_rows
    ids = lax.broadcasted_iota(jnp.int32, (slots, seq_len), 0)
    total = res_ref[0].astype(F32) + dot(gl_ref[0], wg_ref[...], ((1,), (1,)))
    for j in range(early + late_ref.shape[1]):
        hit = (l1_ref[0] - j * slots == ids) | (l2_ref[0] - j * slots == ids)
        hot = jnp.where(hit, 1.0, 0.0).astype(BF16)
        back = early_ref[j] if j < early else late_ref[:, j - early]
        total += dot(hot, back.reshape(slots, hidden), ((0,), (0,)))
    out_ref[0] = total.astype(out_ref.dtype)


def combine(l1, l2, early, late, res, grad_logits, w_gate):
    groups, seq_len, hidden = res.shape
    devices, count, _, cap_rows, _ = late.shape
    slots = (early.shape[0] + count) * devices * cap_rows
    experts = w_gate.shape[1]
    id_spec = pl.BlockSpec((1, 1, seq_len), lambda g: (g, 0, 0))
    row_spec = pl.BlockSpec((1, seq_len, hidden), lambda g: (g, 0, 0))
    return pl.pallas_call(
        combine_body,
        out_shape=jax.ShapeDtypeStruct(res.shape, BF16),
        grid=(groups,),
        in_specs=[
            id_spec, id_spec,
            pl.BlockSpec((early.shape[0], devices, 1, cap_rows, hidden), lambda g: (0, 0, g, 0, 0)),
            pl.BlockSpec((devices, count, 1, cap_rows, hidden), lambda g: (0, 0, g, 0, 0)),
            row_spec, pl.BlockSpec((1, seq_len, experts), lambda g: (g, 0, 0)), pl.BlockSpec((hidden, experts), lambda g: (0, 0)),
        ],
        out_specs=row_spec,
        compiler_params=pltpu.CompilerParams(dimension_semantics=('arbitrary',), vmem_limit_bytes=VMEM_LIMIT),
        cost_estimate=pl.CostEstimate(flops=2 * groups * slots * seq_len * hidden, bytes_accessed=2 * groups * slots * hidden + 6 * res.size, transcendentals=0),
        name='combine',
    )(l1[:, None, :], l2[:, None, :], early, late, res, grad_logits, w_gate)


def copy_body(a_ref, b_ref, a_out, b_out):
    a_out[...] = a_ref[...]
    b_out[...] = b_ref[...]


def settle(a, b):
    cuts = 4
    local = a.shape[0]
    specs = [pl.BlockSpec((1, v.shape[1] // cuts, v.shape[2]), lambda j, q: (j, q, 0)) for v in (a, b)]
    return pl.pallas_call(
        copy_body,
        out_shape=tuple(jax.ShapeDtypeStruct(v.shape, v.dtype) for v in (a, b)),
        grid=(local, cuts),
        in_specs=specs,
        out_specs=tuple(specs),
        compiler_params=pltpu.CompilerParams(dimension_semantics=('arbitrary', 'arbitrary'), vmem_limit_bytes=32 * 1024 * 1024),
        cost_estimate=pl.CostEstimate(flops=1 << 34, bytes_accessed=4 * (a.size + b.size), transcendentals=0),
        name='settle',
    )(a, b)


def reduce_body(part_ref, out_ref, landed, total, send1, recv1, send2, recv2):
    devices = part_ref.shape[0]
    me = lax.axis_index('ep')

    def hop(src, dst, s, r, peer):
        return pltpu.make_async_remote_copy(src_ref=src, dst_ref=dst, send_sem=s, recv_sem=r, device_id=(peer,), device_id_type=pl.DeviceIdType.MESH)

    peers = [(k, lax.rem(me + k, devices), lax.rem(me - k + devices, devices)) for k in range(1, devices)]
    for k, to, _ in peers:
        hop(part_ref.at[to], landed.at[me], send1.at[k], recv1.at[k], to).start()
    landed[me] = part_ref[me]
    for k, to, source in peers:
        hop(part_ref.at[to], landed.at[source], send1.at[k], recv1.at[k], to).wait()
    value = jnp.sum(landed[...], axis=0)
    total[...] = value
    out_ref[me] = value
    for k, to, _ in peers:
        hop(total, out_ref.at[me], send2.at[k], recv2.at[k], to).start()
    for k, to, source in peers:
        hop(total, out_ref.at[source], send2.at[k], recv2.at[k], to).wait()


def all_reduce(part):
    dma = pltpu.SemaphoreType.DMA((part.shape[0],))
    vmem = pl.BlockSpec(memory_space=pltpu.VMEM)
    return pl.pallas_call(
        reduce_body,
        out_shape=jax.ShapeDtypeStruct(part.shape, F32),
        in_specs=[vmem],
        out_specs=vmem,
        scratch_shapes=[pltpu.VMEM(part.shape, F32), pltpu.VMEM(part.shape[1:], F32), dma, dma, dma, dma],
        compiler_params=pltpu.CompilerParams(has_side_effects=True, vmem_limit_bytes=16 * 1024 * 1024),
        cost_estimate=pl.CostEstimate(flops=1 << 22, bytes_accessed=4 * part.size, transcendentals=0),
        name='all_reduce',
    )(part)


def solution(mesh):
    ep_size = mesh.shape['ep']

    def layer_body(x_loc, r_loc, w_gate, w_in_loc, w_out_loc, first_ids, second_ids, keep_ids):
        local_groups, seq_len, hidden = x_loc.shape
        experts = w_gate.shape[1]
        local = experts // ep_size
        cap_rows = 2 * seq_len // experts
        region = local_groups * cap_rows
        tokens_all = local_groups * ep_size * seq_len
        numel = tokens_all * hidden

        first_hot, second_hot, first_count, slot_first, slot_second = route(first_ids, second_ids, keep_ids, experts, cap_rows)

        def slot_of(slot, expert_of):
            return jnp.where(slot >= 0, ((expert_of % local) * ep_size + expert_of // local) * cap_rows + slot, -1)

        l1, l2 = slot_of(slot_first, first_ids), slot_of(slot_second, second_ids)

        logits = jnp.einsum('gsh,he->gse', x_loc, w_gate, preferred_element_type=F32)
        router_prob = jax.nn.softmax(logits, axis=-1)
        gate_first = jnp.sum(router_prob * first_hot, axis=-1)
        gate_second = jnp.sum(router_prob * second_hot, axis=-1)
        gate_sum = gate_first + gate_second
        norm_first = (gate_first / gate_sum).astype(BF16)
        norm_second = (gate_second / gate_sum).astype(BF16)
        slot_ids = jnp.arange(cap_rows, dtype=jnp.int32)
        slot_hot_first = (slot_first[..., None] == slot_ids).astype(BF16)
        slot_hot_second = (slot_second[..., None] == slot_ids).astype(BF16)
        nwin = (jnp.einsum('gse,gsc->egc', first_hot, slot_hot_first * norm_first[..., None], preferred_element_type=F32)
                + jnp.einsum('gse,gsc->egc', second_hot, slot_hot_second * norm_second[..., None], preferred_element_type=F32))
        stats = jnp.concatenate([jnp.sum(first_count, axis=0), jnp.sum(router_prob, axis=(0, 1))])
        nwin_rows = nwin.reshape(ep_size, local, region)
        stat_rows = jnp.broadcast_to(jnp.pad(stats, (0, region - 2 * experts)), (ep_size, 1, region))
        nstat = jnp.concatenate([nwin_rows, stat_rows, jnp.zeros((ep_size, 7 - local, region), F32)], axis=1)
        _, _, _, late, back, dw1, dw2, _, dback, stats = moe(l1, l2, x_loc, r_loc, nstat, w_in_loc, w_out_loc, cap_rows)
        late = lax.all_to_all(late.reshape(ep_size, LATE * region, hidden), 'ep', 0, 0, tiled=True)
        frac_first = stats[local, :experts] / tokens_all
        mean_prob = stats[local, experts:2 * experts] / tokens_all
        dwin = dback[:, :local].reshape(experts, local_groups, cap_rows)
        dot_sum = jnp.einsum('gsh,gsh->', x_loc, r_loc, preferred_element_type=F32) + jnp.sum(nwin * dwin)
        dwin_bf = dwin.astype(BF16)
        d_first = jnp.einsum('gse,egc->gsc', first_hot, dwin_bf, preferred_element_type=F32)
        d_second = jnp.einsum('gse,egc->gsc', second_hot, dwin_bf, preferred_element_type=F32)
        grad_norm_first = jnp.sum(d_first * slot_hot_first, axis=-1)
        grad_norm_second = jnp.sum(d_second * slot_hot_second, axis=-1)
        gate_sq = gate_sum * gate_sum
        grad_gate_first = (grad_norm_first - grad_norm_second) * gate_second / gate_sq
        grad_gate_second = (grad_norm_second - grad_norm_first) * gate_first / gate_sq
        grad_prob = grad_gate_first[..., None] * first_hot + grad_gate_second[..., None] * second_hot + (ALPHA * hidden * experts) * frac_first
        grad_logits = router_prob * (grad_prob - jnp.sum(router_prob * grad_prob, axis=-1, keepdims=True))
        grad_logits_bf = grad_logits.astype(BF16)
        grad_gate_local = jnp.einsum('gse,gsh->eh', grad_logits_bf, x_loc, preferred_element_type=F32)
        lanes = 128
        slice_rows = experts * hidden // (ep_size * lanes)
        part = jnp.concatenate([grad_gate_local.reshape(ep_size, slice_rows, lanes), jnp.full((ep_size, 8, lanes), dot_sum)], axis=1)
        dw1, dw2 = settle(dw1, dw2)
        part, late = lax.optimization_barrier((part, late))
        whole = all_reduce(part)
        grad_gate_w = whole[:, :slice_rows].reshape(experts, hidden).T
        loss_value = whole[0, slice_rows, 0] / numel + ALPHA * experts * jnp.sum(frac_first * mean_prob)

        grad_x = combine(l1, l2, back, late.reshape(ep_size, LATE, local_groups, cap_rows, hidden),
                         r_loc, grad_logits_bf, w_gate)
        return loss_value, grad_x, dw1, dw2, grad_gate_w

    row_spec = P('ep', None, None)
    id_spec = P('ep', None)
    return jax.shard_map(layer_body, mesh=mesh, in_specs=(row_spec, row_spec, P(None, None), row_spec, row_spec, id_spec, id_spec, id_spec), out_specs=(P(), row_spec, row_spec, row_spec, P(None, None)), check_vma=False)
```

```python
import functools

import jax
import jax.numpy as jnp
from jax import lax
from jax.experimental import pallas as pl
from jax.experimental.pallas import tpu as pltpu
from jax.sharding import PartitionSpec as P

ALPHA = 0.01
SOURCES = 4
LATE = 2
ORDER = (14, 15, 1, 6, 7, 8, 9, 10, 11, 4, 5, 12, 13, 2, 3)
FF_TILE = 768
VMEM_LIMIT = 64 * 1024 * 1024 - 128 * 1024
GELU_K = 0.7978845608028654
GELU_C = 0.044715

BF16 = jnp.bfloat16
F32 = jnp.float32


def dot(a, b, contract=((1,), (0,))):
    return lax.dot_general(a, b, (contract, ((), ())), preferred_element_type=F32)


def route(first_ids, second_ids, keep_ids, experts, cap_rows):
    seq_len = first_ids.shape[1]
    expert_ids = jnp.arange(experts, dtype=jnp.int32)
    first_hot = (first_ids[..., None] == expert_ids).astype(BF16)
    second_hot = (second_ids[..., None] == expert_ids).astype(BF16)
    second_kept = second_hot * keep_ids.astype(BF16)[..., None]
    seq_ids = jnp.arange(seq_len, dtype=jnp.int32)
    earlier = (seq_ids[:, None] > seq_ids[None, :]).astype(BF16)
    before_first = jnp.einsum('st,gte->gse', earlier, first_hot, preferred_element_type=F32)
    before_second = jnp.einsum('st,gte->gse', earlier, second_kept, preferred_element_type=F32)
    first_count = jnp.sum(first_hot, axis=1, dtype=F32)
    pos_first = jnp.sum(before_first * first_hot, axis=-1).astype(jnp.int32)
    pos_second = jnp.sum((before_second + first_count[:, None, :]) * second_hot, axis=-1).astype(jnp.int32)
    slot_first = jnp.where(pos_first < cap_rows, pos_first, -1)
    slot_second = jnp.where((keep_ids == 1) & (pos_second < cap_rows), pos_second, -1)
    return first_hot, second_hot, first_count, slot_first, slot_second


def plan_body(local, cap_rows, x_ref, wg_ref, e1_ref, e2_ref, k2_ref, l1_ref, l2_ref, nw_ref, st_ref):
    seq_len, experts = x_ref.shape[1], wg_ref.shape[1]
    devices = experts // local
    e1, e2, k2 = e1_ref[0], e2_ref[0], k2_ref[0]
    logits = dot(wg_ref[...], x_ref[0], ((0,), (1,)))
    top = jnp.exp(logits - jnp.max(logits, axis=0, keepdims=True))
    prob = top / jnp.sum(top, axis=0, keepdims=True)
    ids = lax.broadcasted_iota(jnp.int32, (experts, seq_len), 0)
    hot1 = jnp.where(ids == e1, 1.0, 0.0)
    hot2 = jnp.where(ids == e2, 1.0, 0.0)
    kept2 = jnp.where((ids == e2) & (k2 == 1), 1.0, 0.0)
    square = (seq_len, seq_len)
    earlier = jnp.where(lax.broadcasted_iota(jnp.int32, square, 0) < lax.broadcasted_iota(jnp.int32, square, 1), 1.0, 0.0).astype(BF16)
    count = jnp.sum(hot1, axis=1, keepdims=True)
    pos1 = jnp.sum(dot(hot1.astype(BF16), earlier) * hot1, axis=0, keepdims=True).astype(jnp.int32)
    pos2 = jnp.sum((dot(kept2.astype(BF16), earlier) + count) * hot2, axis=0, keepdims=True).astype(jnp.int32)
    gate1 = jnp.sum(prob * hot1, axis=0, keepdims=True)
    gate2 = jnp.sum(prob * hot2, axis=0, keepdims=True)
    both = gate1 + gate2
    rows = lax.broadcasted_iota(jnp.int32, (cap_rows, seq_len), 0)
    at1 = jnp.where(rows == pos1, 1.0, 0.0).astype(BF16)
    at2 = jnp.where((rows == pos2) & (k2 == 1), 1.0, 0.0).astype(BF16)
    nw_ref[0] = dot((hot1 * (gate1 / both)).astype(BF16), at1, ((1,), (1,))) + dot((hot2 * (gate2 / both)).astype(BF16), at2, ((1,), (1,)))
    lane = lax.broadcasted_iota(jnp.int32, st_ref.shape[1:], 1)
    st_ref[0] = jnp.where(lane == 0, count, jnp.sum(prob, axis=1, keepdims=True))
    l1_ref[0] = jnp.where(pos1 < cap_rows, (lax.rem(e1, local) * devices + e1 // local) * cap_rows + pos1, -1)
    l2_ref[0] = jnp.where((pos2 < cap_rows) & (k2 == 1), (lax.rem(e2, local) * devices + e2 // local) * cap_rows + pos2, -1)


def plan(local, cap_rows, x, w_gate, first_ids, second_ids, keep_ids):
    groups, seq_len, hidden = x.shape
    experts = w_gate.shape[1]
    id_spec = pl.BlockSpec((1, 1, seq_len), lambda g: (g, 0, 0))
    ids = jax.ShapeDtypeStruct((groups, 1, seq_len), jnp.int32)
    return pl.pallas_call(
        functools.partial(plan_body, local, cap_rows),
        out_shape=(ids, ids, jax.ShapeDtypeStruct((groups, experts, cap_rows), F32), jax.ShapeDtypeStruct((groups, experts, 128), F32)),
        grid=(groups,),
        in_specs=[pl.BlockSpec((1, seq_len, hidden), lambda g: (g, 0, 0)), pl.BlockSpec((hidden, experts), lambda g: (0, 0)), id_spec, id_spec, id_spec],
        out_specs=(id_spec, id_spec, pl.BlockSpec((1, experts, cap_rows), lambda g: (g, 0, 0)), pl.BlockSpec((1, experts, 128), lambda g: (g, 0, 0))),
        compiler_params=pltpu.CompilerParams(dimension_semantics=('arbitrary',), vmem_limit_bytes=VMEM_LIMIT),
        cost_estimate=pl.CostEstimate(flops=1 << 32, bytes_accessed=2 * x.size, transcendentals=groups * seq_len * experts),
        name='plan',
    )(x, w_gate, first_ids[:, None, :], second_ids[:, None, :], keep_ids[:, None, :])


def moe_body(ff_tile, l1_ref, l2_ref, xg_ref, rg_ref, nstat_ref, w1_ref, w2_ref, send_ref, recv_ref, dxs_ref, late_ref, back_ref, dw1_ref, dw2_ref, dsend_ref, dback_ref, stat_ref,
             w1_buf, w2_buf, acc1, acc2, tile, dx_tile, nrecv, dwin,
             in_send, in_recv, out_send, out_recv, n_send, n_recv, d_send, d_recv, w_sem, x_sem, dx_sem, dw_sem, own_sem, load_sem):
    local, devices, _, groups, cap_rows, hidden = send_ref.shape
    window = groups * cap_rows
    seq_len = xg_ref.shape[1]
    ff = w1_ref.shape[2]
    early = dxs_ref.shape[0]
    rows = SOURCES * window
    tiles = devices // SOURCES
    me = lax.axis_index('ep')

    core, chip = lax.rem(me, 2), me // 2
    bits = [lax.rem(chip // b, 2) for b in (1, 2, 4)]

    def peer_of(k):
        out = me + (1 - 2 * core) * (k % 2)
        for n, bit in enumerate(bits):
            out = out + 2 ** (n + 1) * (1 - 2 * bit) * (k // 2 ** (n + 1) % 2)
        return out

    def remote(src, dst, s, r, peer):
        return pltpu.make_async_remote_copy(src_ref=src, dst_ref=dst, send_sem=s, recv_sem=r, device_id=(peer,), device_id_type=pl.DeviceIdType.MESH)

    def in_copy(j, k, peer):
        return remote(send_ref.at[j, peer], recv_ref.at[j, me], in_send.at[j, k], in_recv.at[j, k], peer)

    def in_landing(j, k, peer):
        return remote(send_ref.at[j, peer], recv_ref.at[j, peer], in_send.at[j, k], in_recv.at[j, k], peer)

    def out_copy(j, k, peer):
        return remote(dxs_ref.at[j, peer], back_ref.at[j, me], out_send.at[j, k], out_recv.at[j, k], peer)

    def out_landing(j, k, peer):
        return remote(dxs_ref.at[j, peer], back_ref.at[j, peer], out_send.at[j, k], out_recv.at[j, k], peer)

    def n_copy(k, peer):
        return remote(nstat_ref.at[peer], nrecv.at[me], n_send.at[k], n_recv.at[k], peer)

    def n_landing(k, peer):
        return remote(nstat_ref.at[peer], nrecv.at[peer], n_send.at[k], n_recv.at[k], peer)

    def d_copy(k, peer):
        return remote(dsend_ref.at[peer], dback_ref.at[me], d_send.at[k], d_recv.at[k], peer)

    def d_landing(k, peer):
        return remote(dsend_ref.at[peer], dback_ref.at[peer], d_send.at[k], d_recv.at[k], peer)

    def each_peer(fn):
        for k in ORDER:
            fn(k, peer_of(k))

    def start_in(j):
        each_peer(lambda k, peer: in_copy(j, k, peer).start())

    def members(t):
        on = [jnp.where(t == 3 - n, 1, 0) for n in range(3)]
        near = chip + sum(2 ** n * (1 - 2 * bits[n]) * on[n] for n in range(3))
        key = sum(2 ** n * on[n] for n in range(3))
        out = []
        for c, q in ((7 - near, 7 - key), (near, key)):
            out += [(2 * q, 2 * c + core), (2 * q + 1, 2 * c + 1 - core)]
        return out

    def weight_copies(j, slot):
        return (pltpu.make_async_copy(w1_ref.at[j], w1_buf.at[slot], w_sem.at[slot, 0]),
                pltpu.make_async_copy(w2_ref.at[j], w2_buf.at[slot], w_sem.at[slot, 1]))

    def tile_copy(j, s, p, ref):
        return pltpu.make_async_copy(ref.at[j, s], tile.at[p], x_sem.at[p])

    def grad_copies(j, slot):
        return (pltpu.make_async_copy(w1_buf.at[slot], dw1_ref.at[j], dw_sem.at[slot, 0]),
                pltpu.make_async_copy(w2_buf.at[slot], dw2_ref.at[j], dw_sem.at[slot, 1]))

    each_peer(lambda k, peer: n_copy(k, peer).start())
    own = pltpu.make_async_copy(nstat_ref.at[me], nrecv.at[me], own_sem)
    own.start()

    held = w2_buf.shape[1] // seq_len
    x_at = [w2_buf.at[g // held, pl.ds(g % held * seq_len, seq_len)] for g in range(groups)]
    wide = ff // hidden
    r_at = [w1_buf.at[g // wide, pl.ds(0, seq_len), pl.ds(g % wide * hidden, hidden)] for g in range(groups)]
    loads = [(pltpu.make_async_copy(xg_ref.at[g], x_at[g], load_sem.at[g, 0]), pltpu.make_async_copy(rg_ref.at[g], r_at[g], load_sem.at[g, 1])) for g in range(groups)]
    for pair in loads:
        for copy in pair:
            copy.start()
    slots = devices * cap_rows
    ids = lax.broadcasted_iota(jnp.int32, (slots, seq_len), 0)

    @pl.loop(0, local)
    def _(j):
        def placed(g, k):
            return pltpu.make_async_copy(dx_tile.at[g % 2, k], send_ref.at[j, :, k, g], dx_sem.at[g % 2 * 2 + k])

        for g in range(groups):
            @pl.when(j == 0)
            def _():
                for copy in loads[g]:
                    copy.wait()

            hit = (l1_ref[g] - j * slots == ids) | (l2_ref[g] - j * slots == ids)
            hot = jnp.where(hit, 1.0, 0.0).astype(BF16)
            for k, src in enumerate((x_at[g], r_at[g])):
                value = dot(hot, src[...]).astype(BF16).reshape(devices, cap_rows, hidden)
                if g >= 2:
                    placed(g - 2, k).wait()
                dx_tile[g % 2, k] = value
                placed(g, k).start()
        for g in (groups - 2, groups - 1):
            for k in range(2):
                placed(g, k).wait()
        start_in(j)

    for copy in weight_copies(0, 0):
        copy.start()
    own.wait()
    each_peer(lambda k, peer: n_landing(k, peer).wait())
    stat_ref[...] = jnp.sum(nrecv[...], axis=0)
    diag = lax.broadcasted_iota(jnp.int32, (window, window), 0) == lax.broadcasted_iota(jnp.int32, (window, window), 1)

    @pl.loop(0, local * tiles)
    def _(i):
        j = i // tiles
        t = lax.rem(i, tiles)
        wslot = lax.rem(j, 2)
        slot = lax.rem(i, 2)
        sources = members(t)

        @pl.when(t == 0)
        def _():
            for copy in weight_copies(j, wslot):
                copy.wait()
            acc1[...] = jnp.zeros_like(acc1)
            acc2[...] = jnp.zeros_like(acc2)

        @pl.when((t == 1) & (j > 0))
        def _():
            for copy in grad_copies(j - 1, 1 - wslot):
                copy.wait()

        @pl.when((t == 1) & (j + 1 < local))
        def _():
            for copy in weight_copies(j + 1, 1 - wslot):
                copy.start()

        for p, (k, s) in enumerate(sources):
            if p == 2:
                @pl.when(t == 0)
                def _():
                    tile_copy(j, s, p, send_ref).start()

                @pl.when(t > 0)
                def _():
                    in_landing(j, k, s).wait_recv()
                    tile_copy(j, s, p, recv_ref).start()
            else:
                in_landing(j, k, s).wait_recv()
                tile_copy(j, s, p, recv_ref).start()
        for p, (k, s) in enumerate(sources):
            tile_copy(j, s, p, recv_ref).wait()

        x = tile[:, 0].reshape(rows, hidden)
        r = tile[:, 1].reshape(rows, hidden).astype(F32)
        weights = [jnp.sum(jnp.where(diag, nrecv[s, pl.ds(j, 1), :], 0.0), axis=1, keepdims=True) for _, s in sources]
        g = (r * jnp.concatenate(weights, axis=0)).astype(BF16)
        h = None
        dx = None
        for f0 in range(0, ff, ff_tile):
            w1 = w1_buf[wslot, :, f0:f0 + ff_tile]
            w2 = w2_buf[wslot, f0:f0 + ff_tile, :]
            pre = dot(x, w1)
            sq = pre * pre
            th = jnp.tanh(pre * (GELU_K + (GELU_K * GELU_C) * sq))
            half = 0.5 + 0.5 * th
            act = (pre * half).astype(BF16)
            slope = half + (0.5 * pre) * (1.0 - th * th) * (GELU_K + (3.0 * GELU_K * GELU_C) * sq)
            ga = dot(g, w2, ((1,), (1,))).astype(BF16).astype(F32)
            gp = (ga * slope).astype(BF16)
            hp = dot(act, w2)
            h = hp if h is None else h + hp
            dp = dot(gp, w1, ((1,), (1,)))
            dx = dp if dx is None else dx + dp
            acc1[:, f0:f0 + ff_tile] += dot(x, gp, ((0,), (0,)))
            acc2[f0:f0 + ff_tile, :] += dot(act, g, ((0,), (0,)))
        dx_tile[slot] = dx.astype(BF16).reshape(dx_tile.shape[1:])
        def store(p, dst):
            return pltpu.make_async_copy(dx_tile.at[slot, p // 2, pl.ds(p % 2 * groups, groups)], dst, dx_sem.at[p])

        @pl.when(j < early)
        def _():
            for p, (_, s) in enumerate(sources):
                if p == 2:
                    @pl.when(t == 0)
                    def _():
                        store(p, back_ref.at[j, me]).start()

                    @pl.when(t > 0)
                    def _():
                        store(p, dxs_ref.at[j, s]).start()
                else:
                    store(p, dxs_ref.at[j, s]).start()

        @pl.when(j >= early)
        def _():
            for p, (_, s) in enumerate(sources):
                store(p, late_ref.at[s, j - early]).start()

        d = jnp.sum(r * h.astype(BF16).astype(F32), axis=1, keepdims=True)
        for p, (_, s) in enumerate(sources):
            dwin[s, pl.ds(j, 1), :] = jnp.sum(jnp.where(diag, d[p * window:(p + 1) * window], 0.0), axis=0, keepdims=True)
        for p, (k, s) in enumerate(sources):
            store(p, late_ref.at[s, 0]).wait()
            if p == 2:
                @pl.when((j < early) & (t > 0))
                def _():
                    out_copy(j, k, s).start()
            else:
                @pl.when(j < early)
                def _():
                    out_copy(j, k, s).start()

        @pl.when(t == tiles - 1)
        def _():
            w1_buf[wslot] = acc1[...].astype(BF16)
            w2_buf[wslot] = acc2[...].astype(BF16)
            for copy in grad_copies(j, wslot):
                copy.start()

    saved = pltpu.make_async_copy(dwin, dsend_ref, own_sem)
    saved.start()
    saved.wait()
    each_peer(lambda k, peer: d_copy(k, peer).start())
    own = pltpu.make_async_copy(dwin.at[me], dback_ref.at[me], own_sem)
    own.start()
    own.wait()
    for copy in grad_copies(local - 1, (local - 1) % 2):
        copy.wait()
    each_peer(lambda k, peer: d_landing(k, peer).wait())

    @pl.loop(0, local)
    def _(j):
        each_peer(lambda k, peer: in_copy(j, k, peer).wait_send())

        @pl.when(j < early)
        def _():
            each_peer(lambda k, peer: out_landing(j, k, peer).wait())


def moe(l1, l2, x, r, nstat, w_in, w_out, cap_rows):
    local, hidden, ff = w_in.shape
    devices = nstat.shape[0]
    groups = x.shape[0]
    early = local - LATE
    anywhere = pl.BlockSpec(memory_space=pl.ANY)
    vmem = pl.BlockSpec(memory_space=pltpu.VMEM)
    region = (groups, cap_rows, hidden)
    send = jax.ShapeDtypeStruct((local, devices, 2) + region, BF16)
    slots = jax.ShapeDtypeStruct((early, devices) + region, BF16)
    late = jax.ShapeDtypeStruct((devices, LATE) + region, BF16)
    small = jax.ShapeDtypeStruct(nstat.shape, F32)
    dma = pltpu.SemaphoreType.DMA
    rows = devices * groups * cap_rows
    return pl.pallas_call(
        functools.partial(moe_body, FF_TILE),
        out_shape=(
            send, send, slots, late, slots,
            jax.ShapeDtypeStruct(w_in.shape, BF16), jax.ShapeDtypeStruct(w_out.shape, BF16),
            small, small, jax.ShapeDtypeStruct(nstat.shape[1:], F32),
        ),
        in_specs=[vmem] * 2 + [anywhere] * 5,
        out_specs=(anywhere,) * 9 + (vmem,),
        scratch_shapes=[
            pltpu.VMEM((2, hidden, ff), BF16), pltpu.VMEM((2, ff, hidden), BF16),
            pltpu.VMEM((hidden, ff), F32), pltpu.VMEM((ff, hidden), F32),
            pltpu.VMEM((SOURCES, 2) + region, BF16), pltpu.VMEM((2, 2, devices, cap_rows, hidden), BF16),
            pltpu.VMEM(nstat.shape, F32), pltpu.VMEM(nstat.shape, F32),
            dma((local, devices)), dma((local, devices)), dma((early, devices)), dma((early, devices)),
            dma((devices,)), dma((devices,)), dma((devices,)), dma((devices,)),
            dma((2, 2)), dma((SOURCES,)), dma((SOURCES,)), dma((2, 2)), dma, dma((groups, 2)),
        ],
        compiler_params=pltpu.CompilerParams(has_side_effects=True, vmem_limit_bytes=VMEM_LIMIT),
        cost_estimate=pl.CostEstimate(flops=12 * local * rows * hidden * ff, bytes_accessed=8 * local * hidden * ff, transcendentals=local * rows * ff),
        name='moe',
    )(l1, l2, x, r, nstat, w_in, w_out)


def combine_body(l1_ref, l2_ref, early_ref, late_ref, res_ref, gl_ref, wg_ref, out_ref):
    early, devices, _, cap_rows, hidden = early_ref.shape
    seq_len = l1_ref.shape[2]
    slots = devices * cap_rows
    ids = lax.broadcasted_iota(jnp.int32, (slots, seq_len), 0)
    total = res_ref[0].astype(F32) + dot(gl_ref[0], wg_ref[...], ((1,), (1,)))
    for j in range(early + late_ref.shape[1]):
        hit = (l1_ref[0] - j * slots == ids) | (l2_ref[0] - j * slots == ids)
        hot = jnp.where(hit, 1.0, 0.0).astype(BF16)
        back = early_ref[j] if j < early else late_ref[:, j - early]
        total += dot(hot, back.reshape(slots, hidden), ((0,), (0,)))
    out_ref[0] = total.astype(out_ref.dtype)


def combine(l1, l2, early, late, res, grad_logits, w_gate):
    groups, seq_len, hidden = res.shape
    devices, count, _, cap_rows, _ = late.shape
    slots = (early.shape[0] + count) * devices * cap_rows
    experts = w_gate.shape[1]
    id_spec = pl.BlockSpec((1, 1, seq_len), lambda g: (g, 0, 0))
    row_spec = pl.BlockSpec((1, seq_len, hidden), lambda g: (g, 0, 0))
    return pl.pallas_call(
        combine_body,
        out_shape=jax.ShapeDtypeStruct(res.shape, BF16),
        grid=(groups,),
        in_specs=[
            id_spec, id_spec,
            pl.BlockSpec((early.shape[0], devices, 1, cap_rows, hidden), lambda g: (0, 0, g, 0, 0)),
            pl.BlockSpec((devices, count, 1, cap_rows, hidden), lambda g: (0, 0, g, 0, 0)),
            row_spec, pl.BlockSpec((1, seq_len, experts), lambda g: (g, 0, 0)), pl.BlockSpec((hidden, experts), lambda g: (0, 0)),
        ],
        out_specs=row_spec,
        compiler_params=pltpu.CompilerParams(dimension_semantics=('arbitrary',), vmem_limit_bytes=VMEM_LIMIT),
        cost_estimate=pl.CostEstimate(flops=2 * groups * slots * seq_len * hidden, bytes_accessed=2 * groups * slots * hidden + 6 * res.size, transcendentals=0),
        name='combine',
    )(l1, l2, early, late, res, grad_logits, w_gate)


def copy_body(a_ref, b_ref, a_out, b_out):
    a_out[...] = a_ref[...]
    b_out[...] = b_ref[...]


def settle(a, b):
    cuts = 4
    local = a.shape[0]
    specs = [pl.BlockSpec((1, v.shape[1] // cuts, v.shape[2]), lambda j, q: (j, q, 0)) for v in (a, b)]
    return pl.pallas_call(
        copy_body,
        out_shape=tuple(jax.ShapeDtypeStruct(v.shape, v.dtype) for v in (a, b)),
        grid=(local, cuts),
        in_specs=specs,
        out_specs=tuple(specs),
        compiler_params=pltpu.CompilerParams(dimension_semantics=('arbitrary', 'arbitrary'), vmem_limit_bytes=32 * 1024 * 1024),
        cost_estimate=pl.CostEstimate(flops=1 << 34, bytes_accessed=4 * (a.size + b.size), transcendentals=0),
        name='settle',
    )(a, b)


def reduce_body(part_ref, out_ref, landed, total, send1, recv1, send2, recv2):
    devices = part_ref.shape[0]
    me = lax.axis_index('ep')

    def hop(src, dst, s, r, peer):
        return pltpu.make_async_remote_copy(src_ref=src, dst_ref=dst, send_sem=s, recv_sem=r, device_id=(peer,), device_id_type=pl.DeviceIdType.MESH)

    peers = [(k, lax.rem(me + k, devices), lax.rem(me - k + devices, devices)) for k in range(1, devices)]
    for k, to, _ in peers:
        hop(part_ref.at[to], landed.at[me], send1.at[k], recv1.at[k], to).start()
    landed[me] = part_ref[me]
    for k, to, source in peers:
        hop(part_ref.at[to], landed.at[source], send1.at[k], recv1.at[k], to).wait()
    value = jnp.sum(landed[...], axis=0)
    total[...] = value
    out_ref[me] = value
    for k, to, _ in peers:
        hop(total, out_ref.at[me], send2.at[k], recv2.at[k], to).start()
    for k, to, source in peers:
        hop(total, out_ref.at[source], send2.at[k], recv2.at[k], to).wait()


def all_reduce(part):
    dma = pltpu.SemaphoreType.DMA((part.shape[0],))
    vmem = pl.BlockSpec(memory_space=pltpu.VMEM)
    return pl.pallas_call(
        reduce_body,
        out_shape=jax.ShapeDtypeStruct(part.shape, F32),
        in_specs=[vmem],
        out_specs=vmem,
        scratch_shapes=[pltpu.VMEM(part.shape, F32), pltpu.VMEM(part.shape[1:], F32), dma, dma, dma, dma],
        compiler_params=pltpu.CompilerParams(has_side_effects=True, vmem_limit_bytes=16 * 1024 * 1024),
        cost_estimate=pl.CostEstimate(flops=1 << 22, bytes_accessed=4 * part.size, transcendentals=0),
        name='all_reduce',
    )(part)


def solution(mesh):
    ep_size = mesh.shape['ep']

    def layer_body(x_loc, r_loc, w_gate, w_in_loc, w_out_loc, first_ids, second_ids, keep_ids):
        local_groups, seq_len, hidden = x_loc.shape
        experts = w_gate.shape[1]
        local = experts // ep_size
        cap_rows = 2 * seq_len // experts
        region = local_groups * cap_rows
        tokens_all = local_groups * ep_size * seq_len
        numel = tokens_all * hidden

        l1, l2, nwin, marks = plan(local, cap_rows, x_loc, w_gate, first_ids, second_ids, keep_ids)
        nwin = nwin.transpose(1, 0, 2)
        stats = jnp.sum(marks[:, :, :2], axis=0).T.reshape(-1)
        nwin_rows = nwin.reshape(ep_size, local, region)
        stat_rows = jnp.broadcast_to(jnp.pad(stats, (0, region - 2 * experts)), (ep_size, 1, region))
        nstat = jnp.concatenate([nwin_rows, stat_rows, jnp.zeros((ep_size, 7 - local, region), F32)], axis=1)
        _, _, _, late, back, dw1, dw2, _, dback, stats = moe(l1, l2, x_loc, r_loc, nstat, w_in_loc, w_out_loc, cap_rows)
        late = lax.all_to_all(late.reshape(ep_size, LATE * region, hidden), 'ep', 0, 0, tiled=True)
        frac_first = stats[local, :experts] / tokens_all
        mean_prob = stats[local, experts:2 * experts] / tokens_all
        dwin = dback[:, :local].reshape(experts, local_groups, cap_rows)
        first_ids, second_ids, keep_ids, gate_late, dwin = lax.optimization_barrier((first_ids, second_ids, keep_ids, w_gate, dwin))
        first_hot, second_hot, first_count, slot_first, slot_second = route(first_ids, second_ids, keep_ids, experts, cap_rows)
        logits = jnp.einsum('gsh,he->gse', x_loc, gate_late, preferred_element_type=F32)
        router_prob = jax.nn.softmax(logits, axis=-1)
        gate_first = jnp.sum(router_prob * first_hot, axis=-1)
        gate_second = jnp.sum(router_prob * second_hot, axis=-1)
        gate_sum = gate_first + gate_second
        norm_first = (gate_first / gate_sum).astype(BF16)
        norm_second = (gate_second / gate_sum).astype(BF16)
        slot_ids = jnp.arange(cap_rows, dtype=jnp.int32)
        slot_hot_first = (slot_first[..., None] == slot_ids).astype(BF16)
        slot_hot_second = (slot_second[..., None] == slot_ids).astype(BF16)
        dot_sum = jnp.einsum('gsh,gsh->', x_loc, r_loc, preferred_element_type=F32) + jnp.sum(nwin * dwin)
        dwin_bf = dwin.astype(BF16)
        d_first = jnp.einsum('gse,egc->gsc', first_hot, dwin_bf, preferred_element_type=F32)
        d_second = jnp.einsum('gse,egc->gsc', second_hot, dwin_bf, preferred_element_type=F32)
        grad_norm_first = jnp.sum(d_first * slot_hot_first, axis=-1)
        grad_norm_second = jnp.sum(d_second * slot_hot_second, axis=-1)
        gate_sq = gate_sum * gate_sum
        grad_gate_first = (grad_norm_first - grad_norm_second) * gate_second / gate_sq
        grad_gate_second = (grad_norm_second - grad_norm_first) * gate_first / gate_sq
        grad_prob = grad_gate_first[..., None] * first_hot + grad_gate_second[..., None] * second_hot + (ALPHA * hidden * experts) * frac_first
        grad_logits = router_prob * (grad_prob - jnp.sum(router_prob * grad_prob, axis=-1, keepdims=True))
        grad_logits_bf = grad_logits.astype(BF16)
        grad_gate_local = jnp.einsum('gse,gsh->eh', grad_logits_bf, x_loc, preferred_element_type=F32)
        lanes = 128
        slice_rows = experts * hidden // (ep_size * lanes)
        part = jnp.concatenate([grad_gate_local.reshape(ep_size, slice_rows, lanes), jnp.full((ep_size, 8, lanes), dot_sum)], axis=1)
        dw1, dw2 = settle(dw1, dw2)
        part, late = lax.optimization_barrier((part, late))
        whole = all_reduce(part)
        grad_gate_w = whole[:, :slice_rows].reshape(experts, hidden).T
        loss_value = whole[0, slice_rows, 0] / numel + ALPHA * experts * jnp.sum(frac_first * mean_prob)

        grad_x = combine(l1, l2, back, late.reshape(ep_size, LATE, local_groups, cap_rows, hidden),
                         r_loc, grad_logits_bf, w_gate)
        return loss_value, grad_x, dw1, dw2, grad_gate_w

    row_spec = P('ep', None, None)
    id_spec = P('ep', None)
    return jax.shard_map(layer_body, mesh=mesh, in_specs=(row_spec, row_spec, P(None, None), row_spec, row_spec, id_spec, id_spec, id_spec), out_specs=(P(), row_spec, row_spec, row_spec, P(None, None)), check_vma=False)
```
